32 devices in a mesh: gx: 4 (over x, core), gy: 2 (over y), gz: 4 (over z).
Axes of the slice: x: 2, y: 2, z: 4, core: 2. Of those that a mesh axis runs over, the one named last changes fastest.
Arguments:
- features: bfloat16 [4, 2, 8, 128, 128], P('gx', 'gy', 'gz'), may hold values from -24 to 24
- frac: bfloat16 [4, 2, 8, 3, 128], P('gx', 'gy', 'gz'), may hold values from -0.5 to 0.5
- subpoint: int32 [4, 2, 8, 3, 128], P('gx', 'gy', 'gz'), may hold values from 0 to 5
- counts: int32 [4, 2, 8], P('gx', 'gy', 'gz'), may hold values from 32 to 128, as said below
- w_query: bfloat16 [128, 128], replicated, may hold values from -1 to 1
- w_key: bfloat16 [128, 128], replicated, may hold values from -1 to 1
- w_value: bfloat16 [128, 128], replicated, may hold values from -0.5 to 0.5
- rbf_coef: float32 [8], replicated, may hold values from -3 to 3
- w_out: bfloat16 [128, 128], replicated, may hold values from -0.5 to 0.5
- w_charge: bfloat16 [128, 128], replicated, may hold values from -0.5 to 0.5
- mode_weight: bfloat16 [2, 12, 48, 3072], P(None, 'gx', 'gy', 'gz'), may hold values from -18 to 18
- mesh_gain: float32 [128], replicated, may hold values from 0.1 to 1.9
- w_up: bfloat16 [128, 256], replicated, may hold values from -0.5 to 0.5
- w_down: bfloat16 [256, 128], replicated, may hold values from -0.375 to 0.375
Outputs:
- atoms_out: bfloat16 [4, 2, 8, 128, 128], P('gx', 'gy', 'gz')
The draws below stay inside these ranges and needn't reach their ends.
Inputs may be any that keep to these rules, and one draw needn't show every extreme that they name: `counts`: a cell's atoms fill its first slots; at least 32 atoms in every cell, and some cell holds 128.
All inputs are finite; a program needn't handle non-finite values.
Results may differ from the reference program's by a relative error of at most 0.012.
Values may be sent and summed in bfloat16 or wider, within the bound.
No kernel may reach another device: no remote copies, remote signals or barrier semaphores. Data moves between devices by JAX's collectives and lax.ppermute only.
A program may use at most 64 MiB of HBM per device.

```python
import math
import jax
import jax.numpy as jnp
from jax import lax

D = 128
C = 128
FF = 256
A = 128
R = 6
NRBF = 8
NCX = 4
NCY = 2
NCZ = 8
MX = 24
MY = 12
MZ = 48


def projection_pair(key):
    base_key = jax.random.fold_in(key, 7)
    query_w = jax.random.normal(jax.random.fold_in(base_key, 1), (D, D), jnp.float32) / math.sqrt(D)
    key_w = jax.random.normal(jax.random.fold_in(base_key, 3), (D, D), jnp.float32) / math.sqrt(D)
    return (jnp.clip(query_w, -1.0, 1.0), jnp.clip(key_w, -1.0, 1.0))


def draw_w_query(key, part):
    return projection_pair(key)[0].astype(jnp.bfloat16)


def draw_w_key(key, part):
    return projection_pair(key)[1].astype(jnp.bfloat16)


def draw_features(key, part):
    shape_all = (NCX, NCY, NCZ, A, D)
    values = jnp.clip(jax.random.normal(jax.random.fold_in(key, 30), shape_all, jnp.float32), -6.0, 6.0)
    return values.astype(jnp.bfloat16)


def draw_counts(key, part):
    filled = jax.random.randint(jax.random.fold_in(key, 51), (NCX, NCY, NCZ), A // 4, A + 1)
    chosen = jax.random.randint(jax.random.fold_in(key, 52), (), 0, NCX * NCY * NCZ)
    flat_index = lax.broadcasted_iota(jnp.int32, (NCX, NCY, NCZ), 0) * (NCY * NCZ)
    flat_index = flat_index + lax.broadcasted_iota(jnp.int32, (NCX, NCY, NCZ), 1) * NCZ
    flat_index = flat_index + lax.broadcasted_iota(jnp.int32, (NCX, NCY, NCZ), 2)
    return jnp.where(flat_index == chosen, A, filled).astype(jnp.int32)


def draw_mode_weight(key, part):
    shape_all = (2, MY, MZ, C, MX)
    values = jnp.clip(jax.random.normal(jax.random.fold_in(key, 60), shape_all, jnp.float32), -4.0, 4.0)
    values = jnp.clip(values, -18.0, 18.0)
    return values.reshape(2, MY, MZ, C * MX).astype(jnp.bfloat16)


def touch_ends(values, rng, smallest, top_value):
    longest = values.shape.index(max(values.shape))
    spots = []
    for shift in (0, 1):
        where = [jax.random.randint(jax.random.fold_in(rng, axis), (), 0, length) for axis, length in enumerate(values.shape)]
        where[longest] = (where[longest] + shift) % values.shape[longest]
        spots.append(tuple(where))
    return values.at[spots[0]].set(smallest).at[spots[1]].set(top_value)


def shard_levels(stream_key, dims, shards, smallest, largest):
    gain = 1.0
    for dim, parts in shards:
        heights = jax.random.uniform(jax.random.fold_in(jax.random.fold_in(stream_key, 6), dim), (parts,), jnp.float32, smallest / len(shards), largest / len(shards))
        gain = gain * jnp.repeat(jnp.exp(heights), dims[dim] // parts).reshape((-1,) + (1,) * (len(dims) - 1 - dim))
    return gain


def bell_draw(stream_key, dims, deviation, reach, kind=jnp.bfloat16):
    drawn = deviation * jax.random.normal(stream_key, dims, jnp.float32)
    return jnp.clip(drawn, min=-reach, max=reach).astype(kind)


def setup_inputs(seed: int = 0) -> dict:
    key_list = jax.random.split(jax.random.key(seed), 15)
    features = draw_features(jax.random.fold_in(key_list[14], 71), 0)
    frac = jnp.clip(jax.random.uniform(key_list[1], (NCX, NCY, NCZ, 3, A), jnp.float32, -0.5, 0.5) * shard_levels(key_list[1], (NCX, NCY, NCZ, 3, A), ((0, 4), (1, 2), (2, 4)), -0.4, 0.0), -0.5, 0.5).astype(jnp.bfloat16)
    subpoint = touch_ends(jax.random.randint(key_list[2], (NCX, NCY, NCZ, 3, A), 0, R), jax.random.fold_in(key_list[2], 1), 0, R - 1).astype(jnp.int32)
    counts = draw_counts(jax.random.fold_in(key_list[14], 71), 0)
    w_query = draw_w_query(jax.random.fold_in(key_list[14], 71), 0)
    w_key = draw_w_key(jax.random.fold_in(key_list[14], 71), 0)
    w_value = bell_draw(key_list[6], (D, D), D ** -0.5, 0.5)
    rbf_coef = bell_draw(key_list[7], (NRBF,), 1.0, 3.0, jnp.float32)
    w_out = bell_draw(key_list[8], (D, D), D ** -0.5, 0.5)
    w_charge = bell_draw(key_list[9], (D, C), D ** -0.5, 0.5)
    mode_weight = draw_mode_weight(jax.random.fold_in(key_list[14], 71), 0)
    mesh_gain = jnp.clip(1.0 + 0.18 * jax.random.normal(key_list[11], (C,), jnp.float32), 0.1, 1.9)
    w_up = bell_draw(key_list[12], (D, FF), D ** -0.5, 0.5)
    w_down = bell_draw(key_list[13], (FF, D), FF ** -0.5, 0.375)
    return {"features": features, "frac": frac, "subpoint": subpoint, "counts": counts, "w_query": w_query, "w_key": w_key, "w_value": w_value, "rbf_coef": rbf_coef, "w_out": w_out, "w_charge": w_charge, "mode_weight": mode_weight, "mesh_gain": mesh_gain, "w_up": w_up, "w_down": w_down}


OFFSETS = [(step_x, step_y, step_z) for step_x in (-1, 0, 1) for step_y in (-1, 0, 1) for step_z in (-1, 0, 1)]

def radial_bias(dist_sq, rbf_coef):
    bias_total = jnp.zeros_like(dist_sq)
    for basis_index in range(NRBF):
        bias_total = bias_total + rbf_coef[basis_index] * jnp.exp(-(0.08 * 2.0 ** basis_index) * dist_sq)
    return bias_total

def attend(queries, key_rows, value_rows, query_pos, key_pos, key_valid, rbf_coef):
    raw_scores = jnp.einsum('nad,nkd->nak', queries.astype(jnp.float32), key_rows.astype(jnp.float32))
    dist_sq = jnp.zeros_like(raw_scores)
    for coordinate in range(3):
        coord_gap = key_pos[:, coordinate, None, :] - query_pos[:, coordinate, :, None]
        dist_sq = dist_sq + coord_gap * coord_gap
    scores = raw_scores * (1.0 / math.sqrt(D)) + radial_bias(dist_sq, rbf_coef)
    scores = jnp.where(key_valid[:, None, :], scores, -jnp.inf)
    row_top = lax.optimization_barrier(jnp.max(scores, axis=-1, keepdims=True))
    exp_scores = jnp.exp(scores - row_top)
    weights = (exp_scores / lax.optimization_barrier(jnp.sum(exp_scores, axis=-1, keepdims=True))).astype(jnp.bfloat16)
    mixed_rows = jnp.einsum('nak,nkd->nad', weights.astype(jnp.float32), value_rows.astype(jnp.float32))
    return mixed_rows.astype(jnp.bfloat16)

def stencil_weights(subpoint, frac):
    points = jnp.arange(R + 2, dtype=jnp.int32)
    offset = points - 1 - subpoint[..., None]
    shifted = frac.astype(jnp.float32)[..., None]
    lower_w = 0.5 * (0.5 - shifted) ** 2
    centre_w = 0.75 - shifted * shifted
    upper_w = 0.5 * (0.5 + shifted) ** 2
    zeroes = jnp.zeros_like(lower_w)
    return jnp.where(offset == -1, lower_w, jnp.where(offset == 0, centre_w, jnp.where(offset == 1, upper_w, zeroes)))

def combine(weights_dim):
    weight_x = weights_dim[..., 0, :, :]
    weight_y = weights_dim[..., 1, :, :]
    weight_z = weights_dim[..., 2, :, :]
    return weight_x[..., :, None, None] * weight_y[..., None, :, None] * weight_z[..., None, None, :]

def fold_line(blocks, dim_index):
    cell_count = blocks.shape[dim_index]
    head_part = lax.slice_in_dim(blocks, 0, R, axis=dim_index + 1)
    tail_part = lax.slice_in_dim(blocks, R, R + 2, axis=dim_index + 1)
    head_pad = [(0, 0)] * blocks.ndim
    head_pad[dim_index] = (0, 1)
    tail_pad = [(0, 0)] * blocks.ndim
    tail_pad[dim_index] = (1, 0)
    tail_pad[dim_index + 1] = (0, R - 2)
    summed = jnp.pad(head_part, head_pad) + jnp.pad(tail_part, tail_pad)
    shape_now = summed.shape
    merged = summed.reshape(shape_now[:dim_index] + ((cell_count + 1) * R,) + shape_now[dim_index + 2:])
    return lax.slice_in_dim(merged, 0, cell_count * R + 2, axis=dim_index)

def wrap_line(line_data, dim_index):
    inner_len = line_data.shape[dim_index] - 2
    middle = lax.slice_in_dim(line_data, 1, inner_len + 1, axis=dim_index)
    front_rim = lax.slice_in_dim(line_data, inner_len + 1, inner_len + 2, axis=dim_index)
    back_rim = lax.slice_in_dim(line_data, 0, 1, axis=dim_index)
    front_pad = [(0, 0)] * line_data.ndim
    front_pad[dim_index] = (0, inner_len - 1)
    back_pad = [(0, 0)] * line_data.ndim
    back_pad[dim_index] = (inner_len - 1, 0)
    return middle + jnp.pad(front_rim, front_pad) + jnp.pad(back_rim, back_pad)

def line_blocks(line_data, dim_index):
    cell_count = (line_data.shape[dim_index] - 2) // R
    widths = [(0, 0)] * line_data.ndim
    widths[dim_index] = (0, R - 2)
    extended = jnp.pad(line_data, widths)
    shape_now = extended.shape
    reshaped = extended.reshape(shape_now[:dim_index] + (cell_count + 1, R) + shape_now[dim_index + 1:])
    head_part = lax.slice_in_dim(reshaped, 0, cell_count, axis=dim_index)
    tail_part = lax.slice_in_dim(lax.slice_in_dim(reshaped, 1, cell_count + 1, axis=dim_index), 0, 2, axis=dim_index + 1)
    return jnp.concatenate([head_part, tail_part], axis=dim_index + 1)

def neighbour_rows(table_data, index_x, index_y):
    pieces = []
    for step_x, step_y, step_z in OFFSETS:
        plane_rows = lax.dynamic_index_in_dim(table_data, (index_x + step_x) % NCX, 0, keepdims=False)
        line_rows = lax.dynamic_index_in_dim(plane_rows, (index_y + step_y) % NCY, 0, keepdims=False)
        pieces.append(jnp.roll(line_rows, -step_z, axis=0))
    return jnp.stack(pieces, axis=1)

def reference(features, frac, subpoint, counts, w_query, w_key, w_value, rbf_coef, w_out, w_charge, mode_weight, mesh_gain, w_up, w_down):
    slot_index = lax.broadcasted_iota(jnp.int32, (NCX, NCY, NCZ, A), 3)
    valid_mask = slot_index < counts[..., None]
    coords = ((subpoint.astype(jnp.float32) + 0.5 + frac.astype(jnp.float32)) / R).astype(jnp.bfloat16)
    queries = jnp.dot(features, w_query, preferred_element_type=jnp.float32).astype(jnp.bfloat16)
    key_rows = jnp.dot(features, w_key, preferred_element_type=jnp.float32).astype(jnp.bfloat16)
    value_rows = jnp.dot(features, w_value, preferred_element_type=jnp.float32).astype(jnp.bfloat16)
    offsets = jnp.array(OFFSETS, dtype=jnp.float32)

    def plane_block(index_x):

        def line_block(index_y):
            near_keys = neighbour_rows(key_rows, index_x, index_y).reshape(NCZ, 27 * A, D)
            near_values = neighbour_rows(value_rows, index_x, index_y).reshape(NCZ, 27 * A, D)
            near_pos = neighbour_rows(coords, index_x, index_y).astype(jnp.float32) + offsets[None, :, :, None]
            near_pos = jnp.transpose(near_pos, (0, 2, 1, 3)).reshape(NCZ, 3, 27 * A)
            near_valid = neighbour_rows(valid_mask, index_x, index_y).reshape(NCZ, 27 * A)
            own_queries = lax.dynamic_index_in_dim(lax.dynamic_index_in_dim(queries, index_x, 0, keepdims=False), index_y, 0, keepdims=False)
            own_pos = lax.dynamic_index_in_dim(lax.dynamic_index_in_dim(coords, index_x, 0, keepdims=False), index_y, 0, keepdims=False).astype(jnp.float32)
            return attend(own_queries, near_keys, near_values, own_pos, near_pos, near_valid, rbf_coef)
        return lax.map(line_block, jnp.arange(NCY, dtype=jnp.int32))
    attended = lax.map(plane_block, jnp.arange(NCX, dtype=jnp.int32))
    after_attn = features.astype(jnp.float32) + jnp.dot(attended, w_out, preferred_element_type=jnp.float32)
    charges = jnp.dot(features, w_charge, preferred_element_type=jnp.float32) * valid_mask[..., None].astype(jnp.float32)
    weights_dim = stencil_weights(subpoint, frac)

    def deposit(carry, index_x):
        slab_weight = combine(lax.dynamic_index_in_dim(weights_dim, index_x, 0, keepdims=False))
        slab_charge = lax.dynamic_index_in_dim(charges, index_x, 0, keepdims=False)
        blocks = jnp.einsum('yzapqr,yzac->pyqzrc', slab_weight, slab_charge, precision=lax.Precision.HIGHEST)
        folded = wrap_line(fold_line(blocks, 1), 1)
        folded = wrap_line(fold_line(folded, 2), 2)
        current = lax.dynamic_slice_in_dim(carry, R * index_x, R + 2, 0)
        carry = lax.dynamic_update_slice_in_dim(carry, current + folded, R * index_x, 0)
        return (carry, None)
    padded = jnp.zeros((MX + 2, MY, MZ, C), jnp.float32)
    padded, unused = lax.scan(deposit, padded, jnp.arange(NCX, dtype=jnp.int32))
    density = wrap_line(padded, 0)
    mode_full = jnp.transpose(mode_weight.reshape(2, MY, MZ, C, MX), (0, 4, 1, 2, 3))

    def filter_group(index_c):
        first_chan = index_c * 16
        density_part = lax.dynamic_slice_in_dim(density, first_chan, 16, 3)
        real_weight = lax.dynamic_slice_in_dim(mode_full[0], first_chan, 16, 3).astype(jnp.float32)
        imag_weight = lax.dynamic_slice_in_dim(mode_full[1], first_chan, 16, 3).astype(jnp.float32)
        spectrum = jnp.fft.fftn(density_part, axes=(0, 1, 2))
        spectrum = spectrum * (real_weight + 1j * imag_weight)
        return jnp.real(jnp.fft.ifftn(spectrum, axes=(0, 1, 2)))
    potential = lax.map(filter_group, jnp.arange(C // 16, dtype=jnp.int32))
    potential = jnp.moveaxis(potential, 0, 3).reshape(MX, MY, MZ, C)
    padded_pot = jnp.pad(potential, ((1, 1), (1, 1), (1, 1), (0, 0)), mode='wrap')

    def sample_plane(index_x):
        slab_rows = lax.dynamic_slice_in_dim(padded_pot, R * index_x, R + 2, 0)
        blocks = line_blocks(line_blocks(slab_rows, 1), 3)
        slab_weight = combine(lax.dynamic_index_in_dim(weights_dim, index_x, 0, keepdims=False))
        return jnp.einsum('yzapqr,pyqzrc->yzac', slab_weight, blocks, precision=lax.Precision.HIGHEST)
    sampled = lax.map(sample_plane, jnp.arange(NCX, dtype=jnp.int32))
    norm_scale = lax.rsqrt(lax.optimization_barrier(jnp.mean(sampled * sampled, axis=-1, keepdims=True)) + 1e-06)
    joined = after_attn + sampled * norm_scale * mesh_gain
    joined_in = joined.astype(jnp.bfloat16)
    inner_act = jax.nn.silu(jnp.dot(joined_in, w_up, preferred_element_type=jnp.float32)).astype(jnp.bfloat16)
    result = joined + jnp.dot(inner_act, w_down, preferred_element_type=jnp.float32)
    return jnp.where(valid_mask[..., None], result, 0.0).astype(jnp.bfloat16)
```

```python
import math
from functools import partial

import jax
import jax.numpy as jnp
import numpy as np
from jax import lax
from jax.experimental import pallas as pl
from jax.experimental.pallas import tpu as pltpu
from jax.sharding import PartitionSpec as P

D = 128
R = 6
NRBF = 8


OFFSETS = [
    (step_x, step_y, step_z)
    for step_x in (-1, 0, 1)
    for step_y in (-1, 0, 1)
    for step_z in (-1, 0, 1)
]


def padded_2(array, sides, width):
    for axis, dim in sides:
        devices, length = (lax.axis_size(axis), array.shape[dim])
        up = [(i, (i + 1) % devices) for i in range(devices)]
        down = [(j, i) for i, j in up]
        last = lax.slice_in_dim(array, length - width, length, axis=dim)
        first = lax.slice_in_dim(array, 0, width, axis=dim)
        before = lax.ppermute(last, axis, up)
        after = lax.ppermute(first, axis, down)
        array = jnp.concatenate([before, array, after], axis=dim)
    return array


def as_sent(array):
    return jax.tree.map(lambda a: a.astype(jnp.bfloat16) if a.dtype == jnp.float32 else a, array)


def radial_bias(dist_sq, rbf_coef):
    bias_total = jnp.zeros_like(dist_sq)
    for basis_index in range(NRBF):
        bias_total = bias_total + rbf_coef[basis_index] * jnp.exp(
            -(0.08 * 2.0**basis_index) * dist_sq
        )
    return bias_total


def attend(queries, key_rows, value_rows, query_pos, key_pos, key_valid, rbf_coef):
    raw_scores = jnp.einsum("nad,nkd->nak", queries, key_rows, preferred_element_type=jnp.float32)
    dist_sq = jnp.zeros_like(raw_scores)
    for coordinate in range(3):
        coord_gap = key_pos[:, coordinate, None, :] - query_pos[:, coordinate, :, None]
        dist_sq = dist_sq + coord_gap * coord_gap
    scores = raw_scores * (1.0 / math.sqrt(D)) + radial_bias(dist_sq, rbf_coef)
    scores = jnp.where(key_valid[:, None, :], scores, -jnp.inf)
    row_top = jnp.max(scores, axis=-1, keepdims=True)
    exp_scores = jnp.exp(scores - row_top)
    weights = (exp_scores / jnp.sum(exp_scores, axis=-1, keepdims=True)).astype(jnp.bfloat16)
    mixed_rows = jnp.einsum("nak,nkd->nad", weights, value_rows, preferred_element_type=jnp.float32)
    return mixed_rows.astype(jnp.bfloat16)


def stencil_weights(subpoint, frac):
    points = jnp.arange(R + 2, dtype=jnp.int32)
    offset = points - 1 - subpoint[..., None]
    shifted = frac.astype(jnp.float32)[..., None]
    lower_w = 0.5 * (0.5 - shifted) ** 2
    centre_w = 0.75 - shifted * shifted
    upper_w = 0.5 * (0.5 + shifted) ** 2
    zeroes = jnp.zeros_like(lower_w)
    return jnp.where(
        offset == -1,
        lower_w,
        jnp.where(offset == 0, centre_w, jnp.where(offset == 1, upper_w, zeroes)),
    )


def combine(weights_dim):
    weight_x = weights_dim[..., 0, :, :]
    weight_y = weights_dim[..., 1, :, :]
    weight_z = weights_dim[..., 2, :, :]
    return (
        weight_x[..., :, None, None] * weight_y[..., None, :, None] * weight_z[..., None, None, :]
    )


def fold_line(blocks, dim_index):
    cell_count = blocks.shape[dim_index]
    head_part = lax.slice_in_dim(blocks, 0, R, axis=dim_index + 1)
    tail_part = lax.slice_in_dim(blocks, R, R + 2, axis=dim_index + 1)
    head_pad = [(0, 0)] * blocks.ndim
    head_pad[dim_index] = (0, 1)
    tail_pad = [(0, 0)] * blocks.ndim
    tail_pad[dim_index] = (1, 0)
    tail_pad[dim_index + 1] = (0, R - 2)
    summed = jnp.pad(head_part, head_pad) + jnp.pad(tail_part, tail_pad)
    shape_now = summed.shape
    merged = summed.reshape(
        shape_now[:dim_index] + ((cell_count + 1) * R,) + shape_now[dim_index + 2 :]
    )
    return lax.slice_in_dim(merged, 0, cell_count * R + 2, axis=dim_index)


def line_blocks(line_data, dim_index):
    cell_count = (line_data.shape[dim_index] - 2) // R
    widths = [(0, 0)] * line_data.ndim
    widths[dim_index] = (0, R - 2)
    extended = jnp.pad(line_data, widths)
    shape_now = extended.shape
    reshaped = extended.reshape(
        shape_now[:dim_index] + (cell_count + 1, R) + shape_now[dim_index + 1 :]
    )
    head_part = lax.slice_in_dim(reshaped, 0, cell_count, axis=dim_index)
    tail_part = lax.slice_in_dim(
        lax.slice_in_dim(reshaped, 1, cell_count + 1, axis=dim_index), 0, 2, axis=dim_index + 1
    )
    return jnp.concatenate([head_part, tail_part], axis=dim_index + 1)


def fold_margin(extended, dim_index):
    inner_len = extended.shape[dim_index] - 4
    middle = lax.slice_in_dim(extended, 2, inner_len + 2, axis=dim_index)
    front_rim = lax.slice_in_dim(extended, 0, 1, axis=dim_index)
    back_rim = lax.slice_in_dim(extended, inner_len + 3, inner_len + 4, axis=dim_index)
    front_pad = [(0, 0)] * extended.ndim
    front_pad[dim_index] = (0, inner_len - 1)
    back_pad = [(0, 0)] * extended.ndim
    back_pad[dim_index] = (inner_len - 1, 0)
    return middle + jnp.pad(front_rim, front_pad) + jnp.pad(back_rim, back_pad)


def dft_tables(length):
    index_row = lax.broadcasted_iota(jnp.int32, (length, length), 0)
    index_col = lax.broadcasted_iota(jnp.int32, (length, length), 1)
    angle_grid = 2.0 * math.pi / length * (index_row * index_col % length).astype(jnp.float32)
    return (jnp.cos(angle_grid), jnp.sin(angle_grid))


def along_x(field_data, table_data):
    return jnp.einsum("xyzc,xk->kyzc", field_data, table_data, precision=lax.Precision.HIGHEST)


def along_y(field_data, table_data):
    return jnp.einsum("xyzc,yk->xkzc", field_data, table_data, precision=lax.Precision.HIGHEST)


def along_z(field_data, table_data):
    return jnp.einsum("xyzc,zk->xykc", field_data, table_data, precision=lax.Precision.HIGHEST)


def forward_y(pair_data):
    real_part, imag_part = pair_data
    cos_table, sine_table = dft_tables(real_part.shape[1])
    return (
        along_y(real_part, cos_table) + along_y(imag_part, sine_table),
        along_y(imag_part, cos_table) - along_y(real_part, sine_table),
    )


def inverse_y(pair_data):
    real_part, imag_part = pair_data
    cos_table, sine_table = dft_tables(real_part.shape[1])
    return (
        along_y(real_part, cos_table) - along_y(imag_part, sine_table),
        along_y(imag_part, cos_table) + along_y(real_part, sine_table),
    )


def gather_near(slab_rows, cells_y, cells_z):
    pieces = []
    for step_x, step_y, step_z in OFFSETS:
        pieces.append(
            slab_rows[
                step_x + 1, step_y + 1 : step_y + 1 + cells_y, step_z + 1 : step_z + 1 + cells_z
            ]
        )
    return jnp.stack(pieces, axis=2)


def per_device(
    features,
    frac,
    subpoint,
    counts,
    w_query,
    w_key,
    w_value,
    rbf_coef,
    w_out,
    w_charge,
    mode_weight,
    mesh_gain,
    w_up,
    w_down,
):
    cells_x, cells_y, cells_z, slot_count, width_d = features.shape
    slot_index = lax.broadcasted_iota(jnp.int32, (cells_x, cells_y, cells_z, slot_count), 3)
    valid_mask = slot_index < counts[..., None]
    coords = ((subpoint.astype(jnp.float32) + 0.5 + frac.astype(jnp.float32)) / R).astype(
        jnp.bfloat16
    )
    aux_rows = jnp.concatenate([coords, valid_mask.astype(jnp.bfloat16)[:, :, :, None, :]], axis=3)
    queries = jnp.dot(features, w_query, preferred_element_type=jnp.float32).astype(jnp.bfloat16)
    near_feat, near_aux = (
        padded_2(features, (("gx", 0), ("gy", 1), ("gz", 2)), 1),
        padded_2(aux_rows, (("gx", 0), ("gy", 1), ("gz", 2)), 1),
    )
    near_keys = jnp.dot(near_feat, w_key, preferred_element_type=jnp.float32).astype(jnp.bfloat16)
    near_values = jnp.dot(near_feat, w_value, preferred_element_type=jnp.float32).astype(
        jnp.bfloat16
    )
    offsets = jnp.array(OFFSETS, dtype=jnp.float32)
    group_size = cells_y * cells_z

    def plane_block(index_x):
        key_stack = gather_near(near_keys, cells_y, cells_z).reshape(
            group_size, 27 * slot_count, width_d
        )
        value_stack = gather_near(near_values, cells_y, cells_z).reshape(
            group_size, 27 * slot_count, width_d
        )
        pos_stack = gather_near(near_aux, cells_y, cells_z).astype(jnp.float32)
        key_pos = pos_stack[:, :, :, 0:3, :] + offsets[None, None, :, :, None]
        key_pos = jnp.transpose(key_pos, (0, 1, 3, 2, 4)).reshape(group_size, 3, 27 * slot_count)
        key_valid = (pos_stack[:, :, :, 3, :] > 0.5).reshape(group_size, 27 * slot_count)
        own_queries = lax.dynamic_index_in_dim(queries, index_x, 0, keepdims=False).reshape(
            group_size, slot_count, width_d
        )
        own_pos = (
            lax.dynamic_index_in_dim(coords, index_x, 0, keepdims=False)
            .astype(jnp.float32)
            .reshape(group_size, 3, slot_count)
        )
        mixed_rows = attend(
            own_queries, key_stack, value_stack, own_pos, key_pos, key_valid, rbf_coef
        )
        return mixed_rows.reshape(cells_y, cells_z, slot_count, width_d)

    attended = lax.map(plane_block, jnp.arange(cells_x, dtype=jnp.int32))
    after_attn = features.astype(jnp.float32) + jnp.dot(
        attended, w_out, preferred_element_type=jnp.float32
    )
    charges = jnp.dot(features, w_charge, preferred_element_type=jnp.float32) * valid_mask[
        ..., None
    ].astype(jnp.float32)
    chan_all = charges.shape[-1]
    span = R + 2
    cell_total = cells_x * cells_y * cells_z
    block_weight = combine(stencil_weights(subpoint, frac)).reshape(
        cell_total, slot_count, span * span * span
    )
    charge_rows = charges.reshape(cell_total, slot_count, chan_all)
    spread_cells = jnp.einsum(
        "nas,nac->nsc", block_weight, charge_rows, precision=lax.Precision.HIGHEST
    )
    spread_cells = spread_cells.reshape(cells_x, cells_y, cells_z, span, span, span, chan_all)
    blocks = jnp.transpose(spread_cells, (0, 3, 1, 4, 2, 5, 6))
    padded = fold_line(fold_line(fold_line(blocks, 0), 1), 2)
    margin = padded_2(padded.astype(jnp.bfloat16), (("gx", 0), ("gy", 1), ("gz", 2)), 1).astype(
        padded.dtype
    )
    local_density = fold_margin(fold_margin(fold_margin(margin, 0), 1), 2)
    density = lax.all_to_all(
        local_density.astype(jnp.bfloat16), "gz", split_axis=3, concat_axis=2, tiled=True
    ).astype(local_density.dtype)
    mesh_z = density.shape[2]
    mesh_y = density.shape[1] * lax.axis_size("gy")
    mesh_x = density.shape[0] * lax.axis_size("gx")
    cos_z, sin_z = dft_tables(mesh_z)
    inverse_scale = 1.0 / (mesh_x * mesh_y * mesh_z)
    spec_real = along_z(density, cos_z)
    spec_imag = -along_z(density, sin_z)
    spec_real, spec_imag = forward_y(
        (
            lax.all_to_all(
                spec_real.astype(jnp.bfloat16), "gy", split_axis=2, concat_axis=1, tiled=True
            ).astype(spec_real.dtype),
            lax.all_to_all(
                spec_imag.astype(jnp.bfloat16), "gy", split_axis=2, concat_axis=1, tiled=True
            ).astype(spec_imag.dtype),
        )
    )
    spec_real, spec_imag = (
        lax.all_to_all(as_sent(spec_real), "gx", split_axis=1, concat_axis=0, tiled=True).astype(
            spec_real.dtype
        ),
        lax.all_to_all(as_sent(spec_imag), "gx", split_axis=1, concat_axis=0, tiled=True).astype(
            spec_imag.dtype
        ),
    )
    cos_x, sin_x = dft_tables(mesh_x)
    rotated_real = along_x(spec_real, cos_x) + along_x(spec_imag, sin_x)
    rotated_imag = along_x(spec_imag, cos_x) - along_x(spec_real, sin_x)
    chan_local = spec_real.shape[3]
    weight_both = mode_weight.reshape(
        2, mode_weight.shape[1], mode_weight.shape[2], chan_local, mesh_x
    )
    weight_both = jnp.transpose(weight_both, (0, 4, 1, 2, 3)).astype(jnp.float32)
    weight_real = weight_both[0]
    weight_imag = weight_both[1]
    mixed_real = rotated_real * weight_real - rotated_imag * weight_imag
    mixed_imag = rotated_real * weight_imag + rotated_imag * weight_real
    back_real = along_x(mixed_real, cos_x) - along_x(mixed_imag, sin_x)
    back_imag = along_x(mixed_imag, cos_x) + along_x(mixed_real, sin_x)
    back_real, back_imag = inverse_y(
        (
            lax.all_to_all(
                as_sent(back_real), "gx", split_axis=0, concat_axis=1, tiled=True
            ).astype(back_real.dtype),
            lax.all_to_all(
                as_sent(back_imag), "gx", split_axis=0, concat_axis=1, tiled=True
            ).astype(back_imag.dtype),
        )
    )
    real_part = lax.all_to_all(
        as_sent(back_real), "gy", split_axis=1, concat_axis=2, tiled=True
    ).astype(back_real.dtype)
    imag_part = lax.all_to_all(
        as_sent(back_imag), "gy", split_axis=1, concat_axis=2, tiled=True
    ).astype(back_imag.dtype)
    potential = (along_z(real_part, cos_z) - along_z(imag_part, sin_z)) * inverse_scale
    local_pot = lax.all_to_all(
        as_sent(potential), "gz", split_axis=2, concat_axis=3, tiled=True
    ).astype(potential.dtype)
    padded_pot = padded_2(as_sent(local_pot), (("gx", 0), ("gy", 1), ("gz", 2)), 1).astype(
        local_pot.dtype
    )
    near_blocks = line_blocks(line_blocks(line_blocks(padded_pot, 0), 2), 4)
    near_blocks = jnp.transpose(near_blocks, (0, 2, 4, 1, 3, 5, 6)).reshape(
        cell_total, span * span * span, chan_all
    )
    sampled = jnp.einsum("nas,nsc->nac", block_weight, near_blocks, precision=lax.Precision.HIGHEST)
    sampled = sampled.reshape(cells_x, cells_y, cells_z, slot_count, chan_all)
    norm_scale = lax.rsqrt(jnp.mean(sampled * sampled, axis=-1, keepdims=True) + 1e-06)
    joined = after_attn + sampled * norm_scale * mesh_gain
    joined_in = joined.astype(jnp.bfloat16)
    inner_act = jax.nn.silu(jnp.dot(joined_in, w_up, preferred_element_type=jnp.float32)).astype(
        jnp.bfloat16
    )
    result = joined + jnp.dot(inner_act, w_down, preferred_element_type=jnp.float32)
    return jnp.where(valid_mask[..., None], result, 0.0).astype(jnp.bfloat16)


BIG = 1e30
LOG2E = math.log2(math.e)
PACK = 144
VMEM = pl.BlockSpec(memory_space=pltpu.VMEM)
SMEM = pl.BlockSpec(memory_space=pltpu.SMEM)


def stencil(points, sub, shifted):
    offset = points - 1 - sub
    lower_w = 0.5 * (0.5 - shifted) * (0.5 - shifted)
    centre_w = 0.75 - shifted * shifted
    upper_w = 0.5 * (0.5 + shifted) * (0.5 + shifted)
    return jnp.where(
        offset == -1,
        lower_w,
        jnp.where(offset == 0, centre_w, jnp.where(offset == 1, upper_w, 0.0)),
    )


def cell_weights(frac_n, sub_n, cell, z_pad):
    slots = sub_n.shape[-1]
    span = R + 2
    rows = lax.broadcasted_iota(jnp.int32, (span, slots), 0)
    rows_z = lax.broadcasted_iota(jnp.int32, (z_pad, slots), 0)
    weight_x = stencil(rows, sub_n[0:1], frac_n[0:1])
    weight_y = stencil(rows, sub_n[1:2], frac_n[1:2])
    weight_z = stencil(rows_z, sub_n[2:3] + R * cell, frac_n[2:3])
    weight_yz = (weight_y[:, None, :] * weight_z[None, :, :]).reshape(span * z_pad, slots)
    return weight_x, weight_yz


def spread_kernel(cells, z_pad, feat_ref, frac_ref, sub_ref, count_ref, wc_ref, send_ref, pack_ref):
    slots, width = feat_ref.shape[1], feat_ref.shape[2]
    span = R + 2
    wc_t = wc_ref[...].T
    lhs, rhs = [], []
    for n in range(cells):
        frac_n = frac_ref[n].astype(jnp.float32)
        sub_n = sub_ref[n]
        valid = (lax.broadcasted_iota(jnp.int32, (1, slots), 1) < count_ref[n]).astype(jnp.float32)
        weight_x, weight_yz = cell_weights(frac_n, sub_n, n, z_pad)
        charge_t = lax.dot_general(
            wc_t, feat_ref[n], (((1,), (1,)), ((), ())), preferred_element_type=jnp.float32
        )
        charge_t = charge_t * valid
        chans = charge_t.shape[0]
        lhs.append(
            (charge_t[:, None, :] * weight_x[None, :, :])
            .reshape(chans * span, slots)
            .astype(jnp.bfloat16)
        )
        rhs.append(weight_yz.astype(jnp.bfloat16))
        coords = ((sub_n.astype(jnp.float32) + 0.5 + frac_n) / R).astype(jnp.bfloat16)
        aux = jnp.concatenate(
            [
                coords.astype(jnp.float32),
                valid,
                jnp.zeros((PACK - slots - 4, slots), jnp.float32),
            ],
            axis=0,
        )
        pack_ref[n, 0:slots, :] = feat_ref[n]
        pack_ref[n, slots:PACK, :] = aux.astype(jnp.bfloat16)
    block = lax.dot_general(
        jnp.concatenate(lhs, axis=1),
        jnp.concatenate(rhs, axis=1),
        (((1,), (1,)), ((), ())),
        preferred_element_type=jnp.float32,
    )
    send_ref[...] = block.astype(jnp.bfloat16).reshape(send_ref.shape)


def weight_split_kernel(groups, piece, w_ref, out_ref):
    rows = w_ref.shape[0]
    lanes = out_ref.shape[2]
    for g in range(groups):
        part = w_ref[:, g * piece : (g + 1) * piece].astype(jnp.float32)
        if lanes > piece:
            part = jnp.concatenate([part, jnp.zeros((rows, lanes - piece), jnp.float32)], axis=1)
        out_ref[g] = part.astype(jnp.bfloat16)


def spectral_kernel(sizes, scale, d_ref, t_ref, xf_ref, xi_ref, w_ref, out_ref, f_ref):
    nx, ny, nz = sizes
    rows, lanes = d_ref.shape[1], d_ref.shape[2]
    half = t_ref.shape[0] // 2
    data = jnp.concatenate(
        [
            jnp.concatenate([d_ref[(z * nx + x) * ny + y] for x in range(nx)], axis=0)
            for y in range(ny)
            for z in range(nz)
        ],
        axis=1,
    )
    spec = lax.dot_general(
        t_ref[...], data, (((1,), (1,)), ((), ())), preferred_element_type=jnp.float32
    ).astype(jnp.bfloat16)
    both = jnp.concatenate([spec[:half], spec[half:]], axis=1)
    rot = jnp.dot(both, xf_ref[...], preferred_element_type=jnp.float32)
    wide = rot.shape[1] // 2
    sources = w_ref.shape[0]
    piece = w_ref.shape[1] // 2
    for s in range(sources):
        re = rot[s * piece : (s + 1) * piece, :wide]
        im = rot[s * piece : (s + 1) * piece, wide:]
        w_both = w_ref[s].astype(jnp.float32)
        w_re, w_im = w_both[:piece], w_both[piece:]
        f_ref[s * piece : (s + 1) * piece, :wide] = (re * w_re - im * w_im) * scale
        f_ref[s * piece : (s + 1) * piece, wide:] = (re * w_im + im * w_re) * scale
    back = lax.dot_general(
        xi_ref[...],
        f_ref[...].astype(jnp.bfloat16),
        (((1,), (1,)), ((), ())),
        preferred_element_type=jnp.float32,
    ).astype(jnp.bfloat16)
    both_t = jnp.concatenate([back[: rows * nx], back[rows * nx :]], axis=1)
    pot = jnp.dot(both_t, t_ref[...], preferred_element_type=jnp.float32).astype(jnp.bfloat16)
    for y in range(ny):
        for z in range(nz):
            lane = (y * nz + z) * lanes
            for x in range(nx):
                out_ref[(z * nx + x) * ny + y] = pot[x * rows : (x + 1) * rows, lane : lane + lanes]


def attend_kernel(
    cells_z, y_slots, chunk, c_ref, m_ref, p_ref, feat_ref, wq_ref, wk_ref, wv_ref, wo_ref,
    coef_ref, out_ref, k_ref, v_ref, s_ref, q_ref, ci_ref,
):
    slots, width = feat_ref.shape[1], feat_ref.shape[2]
    sides = {-1: m_ref, 0: c_ref, 1: p_ref}
    depth = cells_z + 2
    per_side = (max(y_slots.values()) + 1) * depth
    w_kv = jnp.concatenate([wk_ref[...], wv_ref[...]], axis=1)
    for step_x, ref in sides.items():
        for cell in range(per_side):
            kv = jnp.dot(ref[cell, 0:slots, :], w_kv, preferred_element_type=jnp.float32)
            kv = kv.astype(jnp.bfloat16)
            k_ref[(step_x + 1) * per_side + cell] = kv[:, :width]
            v_ref[(step_x + 1) * per_side + cell] = kv[:, width:]
    coef = [coef_ref[k] * LOG2E for k in range(NRBF)]
    for n in range(cells_z):
        own = y_slots[0] * depth + n + 1
        q_ref[...] = jnp.dot(
            feat_ref[n], wq_ref[...], preferred_element_type=jnp.float32
        ).astype(jnp.bfloat16)
        own_pos = c_ref[own, slots : slots + 16, :].astype(jnp.float32).T
        for axis in range(3):
            ci_ref[axis] = jnp.broadcast_to(own_pos[:, axis : axis + 1], (slots, slots))
        for row in range(0, slots, chunk):
            part = slice(row, row + chunk)
            queries = q_ref[part, :]
            top = jnp.full((chunk, slots), -3.0e38, jnp.float32)
            index = 0
            for step_x in (-1, 0, 1):
                for slot in sorted(set(y_slots.values())):
                    for step_z in (-1, 0, 1):
                        cell = slot * depth + n + 1 + step_z
                        keys = k_ref[(step_x + 1) * per_side + cell]
                        aux = sides[step_x][cell, slots : slots + 16, :].astype(jnp.float32)
                        raw = lax.dot_general(
                            queries, keys, (((1,), (1,)), ((), ())),
                            preferred_element_type=jnp.float32,
                        )
                        raw = raw * (LOG2E / math.sqrt(width)) + (aux[3:4] - 1.0) * BIG
                        gap_x = (aux[0:1] + float(step_x)) - ci_ref[0, part, :]
                        gap_z = (aux[2:3] + float(step_z)) - ci_ref[2, part, :]
                        base = gap_x * gap_x + gap_z * gap_z
                        for step_y in (-1, 0, 1):
                            if y_slots[step_y] != slot:
                                continue
                            gap_y = (aux[1:2] + float(step_y)) - ci_ref[1, part, :]
                            power = jnp.exp2((base + gap_y * gap_y) * (-0.08 * LOG2E))
                            score = raw + coef[0] * power
                            for k in range(1, NRBF):
                                power = power * power
                                score = score + coef[k] * power
                            s_ref[index, part, :] = score
                            top = jnp.maximum(top, score)
                            index += 1
            row_top = jnp.max(top, axis=1, keepdims=True)
            total = jnp.zeros((chunk, slots), jnp.float32)
            mixed = jnp.zeros((chunk, width), jnp.float32)
            index = 0
            for step_x in (-1, 0, 1):
                for slot in sorted(set(y_slots.values())):
                    for step_z in (-1, 0, 1):
                        cell = slot * depth + n + 1 + step_z
                        prob = None
                        for step_y in (-1, 0, 1):
                            if y_slots[step_y] != slot:
                                continue
                            one = jnp.exp2(s_ref[index, part, :] - row_top)
                            prob = one if prob is None else prob + one
                            index += 1
                        total = total + prob
                        mixed = mixed + jnp.dot(
                            prob.astype(jnp.bfloat16), v_ref[(step_x + 1) * per_side + cell],
                            preferred_element_type=jnp.float32,
                        )
            attended = (mixed / jnp.sum(total, axis=1, keepdims=True)).astype(jnp.bfloat16)
            out_ref[n, part, :] = feat_ref[n, part, :].astype(jnp.float32) + jnp.dot(
                attended, wo_ref[...], preferred_element_type=jnp.float32
            )


def finish_kernel(
    cells, z_pad, pot_ref, after_ref, frac_ref, sub_ref, count_ref, gain_ref, up_ref, down_ref,
    out_ref,
):
    slots, width = after_ref.shape[1], after_ref.shape[2]
    span = R + 2
    pot = pot_ref[...].reshape(-1, pot_ref.shape[2])
    for n in range(cells):
        weight_x, weight_yz = cell_weights(
            frac_ref[n].astype(jnp.float32), sub_ref[n], n, z_pad
        )
        lines = jnp.dot(pot, weight_yz.astype(jnp.bfloat16), preferred_element_type=jnp.float32)
        lines = lines.reshape(-1, span, slots) * weight_x[None, :, :]
        sampled = jnp.sum(lines, axis=1).T
        mean_sq = jnp.mean(sampled * sampled, axis=1, keepdims=True)
        joined = after_ref[n] + sampled * lax.rsqrt(mean_sq + 1e-06) * gain_ref[...]
        inner = jnp.dot(
            joined.astype(jnp.bfloat16), up_ref[...], preferred_element_type=jnp.float32
        )
        inner = (inner * (1.0 / (1.0 + jnp.exp(-inner)))).astype(jnp.bfloat16)
        result = joined + jnp.dot(inner, down_ref[...], preferred_element_type=jnp.float32)
        slot_index = lax.broadcasted_iota(jnp.int32, (slots, width), 0)
        out_ref[n] = jnp.where(slot_index < count_ref[n], result, 0.0).astype(jnp.bfloat16)


def transform_tables(mesh_sizes, devices, blocks, parts, chans, z_pad, lane_pad):
    mesh_x, mesh_y, mesh_z = mesh_sizes
    dev_x, dev_y, dev_z = devices
    block_x, block_y, block_z = blocks
    part_y, part_z = parts
    ky = np.arange(mesh_y).reshape(mesh_y // part_y, 1, part_y, 1)
    kz = np.arange(mesh_z).reshape(1, mesh_z // part_z, 1, part_z)
    ky = np.broadcast_to(ky, (mesh_y // part_y, mesh_z // part_z, part_y, part_z)).reshape(-1, 1)
    kz = np.broadcast_to(kz, (mesh_y // part_y, mesh_z // part_z, part_y, part_z)).reshape(-1, 1)
    y = block_y * np.arange(dev_y)[:, None] + np.arange(block_y + 2) - 1
    z = block_z * np.arange(dev_z)[:, None] + np.arange(z_pad) - 1
    shape = (dev_y, dev_z, block_y + 2, z_pad)
    inside = np.broadcast_to(np.arange(z_pad) < block_z + 2, shape).reshape(1, -1)
    y = np.broadcast_to(y[:, None, :, None], shape).reshape(1, -1) % mesh_y
    z = np.broadcast_to(z[None, :, None, :], shape).reshape(1, -1) % mesh_z
    angle = 2.0 * np.pi * ((ky * y % mesh_y) / mesh_y + (kz * z % mesh_z) / mesh_z)
    table = np.concatenate([np.cos(angle) * inside, -np.sin(angle) * inside], axis=0)
    x = (block_x * np.arange(dev_x)[:, None] + np.arange(block_x + 2) - 1) % mesh_x
    kx = np.arange(mesh_x)
    phase = 2.0 * np.pi / mesh_x * (x[:, :, None] * kx % mesh_x)
    same = np.eye(chans)
    cos_x = np.einsum("dxk,ce->dcxek", np.cos(phase), same)
    sin_x = np.einsum("dxk,ce->dcxek", np.sin(phase), same)
    rows = dev_x * chans * (block_x + 2)
    pad = ((0, 0), (0, lane_pad - chans * mesh_x))
    cos_x = np.pad(cos_x.reshape(rows, chans * mesh_x), pad)
    sin_x = np.pad(sin_x.reshape(rows, chans * mesh_x), pad)
    forward = np.block([[cos_x, -sin_x], [sin_x, cos_x]])
    inverse = np.block([[cos_x, -sin_x], [sin_x, cos_x]])
    return tuple(jnp.asarray(t.astype(np.float32)).astype(jnp.bfloat16) for t in (table, forward, inverse))


def shifted_pair(array, axis, low, high):
    devices = lax.axis_size(axis)
    if devices == 1:
        return high, low
    up = [(i, (i + 1) % devices) for i in range(devices)]
    down = [(j, i) for i, j in up]
    return lax.ppermute(high, axis, up), lax.ppermute(low, axis, down)


def per_device_direct(
    features, frac, subpoint, counts, w_query, w_key, w_value, rbf_coef, w_out, w_charge,
    mode_weight, mesh_gain, w_up, w_down,
):
    cells_x, cells_y, cells_z, slots, width = features.shape
    dev_x, dev_y, dev_z = (lax.axis_size(a) for a in ("gx", "gy", "gz"))
    devices = dev_x * dev_y * dev_z
    span = R + 2
    chan_all = w_charge.shape[1]
    chans = chan_all // devices
    mesh_x, mesh_y, mesh_z = (R * cells_x * dev_x, R * cells_y * dev_y, R * cells_z * dev_z)
    z_pad = padded_z(cells_z)
    bf16, f32 = jnp.bfloat16, jnp.float32

    feat = features.reshape(cells_z, slots, width)
    frac_n = frac.reshape(cells_z, 3, slots)
    sub_n = subpoint.reshape(cells_z, 3, slots)
    count_n = counts.reshape(cells_z)

    send, packed = pl.pallas_call(
        partial(spread_kernel, cells_z, z_pad),
        out_shape=(
            jax.ShapeDtypeStruct((devices, chans * span, span * z_pad), bf16),
            jax.ShapeDtypeStruct((cells_z, PACK, width), bf16),
        ),
        in_specs=[VMEM, VMEM, VMEM, SMEM, VMEM],
        out_specs=(VMEM, VMEM),
        name="spread",
    )(feat, frac_n, sub_n, count_n, w_charge)
    order = ("gz", "gx", "gy")
    mesh_block = lax.all_to_all(send, order, split_axis=0, concat_axis=0, tiled=True)

    part_y, part_z = mode_weight.shape[1], mode_weight.shape[2]
    groups = dev_x * dev_y
    piece = chans * mesh_x
    lane_pad = -(-piece // 128) * 128
    w_rows = mode_weight.reshape(2 * part_y * part_z, groups * piece)
    w_send = pl.pallas_call(
        partial(weight_split_kernel, groups, piece),
        out_shape=jax.ShapeDtypeStruct((groups, 2 * part_y * part_z, lane_pad), bf16),
        in_specs=[VMEM],
        out_specs=VMEM,
        name="weight_split",
    )(w_rows)
    w_modes = lax.all_to_all(w_send, ("gx", "gy"), split_axis=0, concat_axis=0, tiled=True)

    below, above = shifted_pair(packed, "gz", packed[0:1], packed[cells_z - 1 : cells_z])
    column = jnp.concatenate([below, packed, above], axis=0)
    if dev_y == 1:
        y_slots, plane = {-1: 0, 0: 0, 1: 0}, column
    elif dev_y == 2:
        other = lax.ppermute(column, "gy", [(0, 1), (1, 0)])
        y_slots, plane = {-1: 1, 0: 0, 1: 1}, jnp.concatenate([column, other], axis=0)
    else:
        before, after = shifted_pair(column, "gy", column, column)
        y_slots = {-1: 0, 0: 1, 1: 2}
        plane = jnp.concatenate([before, column, after], axis=0)
    left, right = shifted_pair(plane, "gx", plane, plane)

    table, x_forward, x_inverse = transform_tables(
        (mesh_x, mesh_y, mesh_z),
        (dev_x, dev_y, dev_z),
        (R * cells_x, R * cells_y, R * cells_z),
        (part_y, part_z),
        chans,
        z_pad,
        lane_pad,
    )
    pot_send = pl.pallas_call(
        partial(spectral_kernel, (dev_x, dev_y, dev_z), 1.0 / (mesh_x * mesh_y * mesh_z)),
        out_shape=jax.ShapeDtypeStruct(send.shape, bf16),
        in_specs=[VMEM] * 5,
        out_specs=VMEM,
        scratch_shapes=[pltpu.VMEM((table.shape[0] // 2, 2 * lane_pad), f32)],
        name="spectral",
    )(mesh_block, table, x_forward, x_inverse, w_modes)
    pot_block = lax.all_to_all(pot_send, order, split_axis=0, concat_axis=0, tiled=True)

    plane_cells = plane.shape[0]
    after_attn = pl.pallas_call(
        partial(attend_kernel, cells_z, y_slots, ATTEND_ROWS),
        out_shape=jax.ShapeDtypeStruct((cells_z, slots, width), f32),
        in_specs=[VMEM] * 8 + [SMEM],
        out_specs=VMEM,
        scratch_shapes=[
            pltpu.VMEM((3 * plane_cells, slots, width), bf16),
            pltpu.VMEM((3 * plane_cells, slots, width), bf16),
            pltpu.VMEM((27, slots, slots), f32),
            pltpu.VMEM((slots, width), bf16),
            pltpu.VMEM((3, slots, slots), f32),
        ],
        cost_estimate=pl.CostEstimate(
            flops=4_000_000_000, bytes_accessed=8_000_000, transcendentals=2_000_000
        ),
        name="attend",
    )(plane, left, right, feat, w_query, w_key, w_value, w_out, rbf_coef)

    result = pl.pallas_call(
        partial(finish_kernel, cells_z, z_pad),
        out_shape=jax.ShapeDtypeStruct((cells_z, slots, width), bf16),
        in_specs=[VMEM] * 4 + [SMEM] + [VMEM] * 3,
        out_specs=VMEM,
        name="finish",
    )(pot_block, after_attn, frac_n, sub_n, count_n, mesh_gain.reshape(1, width), w_up, w_down)
    return result.reshape(features.shape)


ATTEND_ROWS = 64


def padded_z(cells_z):
    return -(-(R * cells_z + 2) // 16) * 16


def direct_fits(mesh, features, w_charge):
    dev_x, dev_y, dev_z = (mesh.shape[a] for a in ("gx", "gy", "gz"))
    cells_x, cells_y, cells_z = (
        features.shape[0] // dev_x,
        features.shape[1] // dev_y,
        features.shape[2] // dev_z,
    )
    devices = dev_x * dev_y * dev_z
    points = R**2 * features.shape[1] * features.shape[2]
    lanes = (R + 2) * padded_z(cells_z)
    return (
        cells_x == 1
        and cells_y == 1
        and w_charge.shape[1] % devices == 0
        and lanes == 128
        and points * dev_y * dev_z * lanes <= 1 << 20
    )


def solution(mesh):
    def whole(*args):
        path = per_device_direct if direct_fits(mesh, args[0], args[9]) else per_device
        return jax.shard_map(
            path,
            mesh=mesh,
            in_specs=(
                P("gx", "gy", "gz", None, None),
                P("gx", "gy", "gz", None, None),
                P("gx", "gy", "gz", None, None),
                P("gx", "gy", "gz"),
                P(),
                P(),
                P(),
                P(),
                P(),
                P(),
                P(None, "gx", "gy", "gz"),
                P(),
                P(),
                P(),
            ),
            out_specs=P("gx", "gy", "gz", None, None),
            check_vma=False,
        )(*args)

    return whole
```
